32 devices in a mesh: wide: 16 (over z, y, core), narrow: 2 (over x).
Axes of the slice: x: 2, y: 2, z: 4, core: 2. Of those that a mesh axis runs over, the one named last changes fastest.
Arguments:
- src_field: bfloat16 [2, 16, 65536], P(None, 'narrow', 'wide'), may hold values from -6 to 6
- src_depth: int32 [65536], P(('wide', 'narrow')), may hold values from 0 to 16, as said below
- packed_counts: int32 [4096, 64, 128], P(('wide', 'narrow')), may hold values from 0 to 100664832, as said below
- pair_source: int32 [4096], P(('wide', 'narrow')), may hold values from 0 to 15
- pair_home: int32 [4096], P(('wide', 'narrow')), may hold values from 0 to 1023, as said below
- pair_count: int32 [32], P(('wide', 'narrow')), may hold values from 64 to 128, as said below
Outputs:
- remapped: bfloat16 [2, 16, 131072], P(None, 'narrow', 'wide')
The draws below stay inside these ranges and needn't reach their ends.
Inputs may be any that keep to these rules, and one draw needn't show every extreme that they name: `src_depth`: depth 0 marks a dry source cell. `packed_counts`: word (p, i, j) holds count (p, i, j) plus 65536 times count (p, i + 64, j); every count lies between 0 and 1536. The target block pair_home[p] is held by wide index pair_home[p] // 64, which differs by at most 2, counted cyclically over the wide axis, from the wide index of the device that holds pair p. Among the 128 pairs of one device at most 51 have target blocks on one wide index, and on some wide index exactly 51 live pairs of that device. A device's pairs from position pair_count[d] on are padding; some device has all 128 live.
All inputs are finite; a program needn't handle non-finite values.
Results may differ from the reference program's by a relative error of at most 0.0054.
Values may be sent and summed in bfloat16 or wider, within the bound.
No kernel may reach another device: no remote copies, remote signals or barrier semaphores. Data moves between devices by JAX's collectives and lax.ppermute only.
A program may use at most 64 MiB of HBM per device.

```python
import jax
import jax.numpy as jnp
from jax import lax

BLK = 128
LEV = 16
VARS = 2
DENOM = 256
REACH = 2
SB_DEV = 16
P_DEV = 128
TB_DEV = 64
CAP = 51
PAIRS = 4096
SRC_CELLS = 65536
N_WIDE = 16
N_NARROW = 2


def draw_src_depth(key, part):
    key = jax.random.fold_in(key, 404)
    key_land, key_depth = jax.random.split(key)
    blocks = SB_DEV * N_WIDE * N_NARROW
    sea_mask = (jax.random.randint(key_land, (blocks, 1), 0, 5) >= 3).astype(jnp.int32)
    cell_depth = jax.random.randint(key_depth, (blocks, BLK), 1, LEV + 1)
    return (cell_depth * sea_mask).reshape(blocks * BLK).astype(jnp.int32)


def draw_packed_counts(key, part):
    key = jax.random.fold_in(key, 101)
    half_rows = BLK // 2
    key_list = jax.random.split(key, 6)
    array_shape = (P_DEV * N_WIDE * N_NARROW, half_rows, BLK)
    row_ids = jnp.arange(half_rows, dtype=jnp.int32)[:, None]
    column_ids = jnp.arange(BLK, dtype=jnp.int32)[None, :]

    def half_counts(key_spread, key_power, key_factor, offset):
        spread = jax.random.randint(key_spread, array_shape, 0, 4)
        exponent = jax.random.randint(key_power, (array_shape[0], half_rows, 1), 0, 10)
        factor = jax.random.randint(key_factor, (array_shape[0], half_rows, 1), 1, 4)
        diagonal = jnp.power(2, exponent) * factor
        on_diagonal = (column_ids == row_ids + offset)[None, :, :]
        return jnp.where(on_diagonal, diagonal, spread)
    lower_half = half_counts(key_list[0], key_list[1], key_list[2], 0)
    upper_half = half_counts(key_list[3], key_list[4], key_list[5], half_rows)
    return (lower_half + 65536 * upper_half).astype(jnp.int32)


def draw_pair_home(key, part):
    key = jax.random.fold_in(key, 202)
    devices = N_WIDE * N_NARROW
    offset_total = 2 * REACH + 1
    key_rows, key_place = jax.random.split(key)
    head_rows = P_DEV // 2
    slot_ids = jnp.arange(offset_total * CAP, dtype=jnp.int32) // CAP
    wide_of = jnp.arange(devices, dtype=jnp.int32) // N_NARROW

    def one_device(row_key, wide_index):
        key_order, key_head, key_tail = jax.random.split(row_key, 3)
        offset_order = jax.random.permutation(key_order, offset_total).astype(jnp.int32)
        wanted = offset_order[slot_ids][:P_DEV]
        ordering = jnp.concatenate([jax.random.permutation(key_head, head_rows), head_rows + jax.random.permutation(key_tail, P_DEV - head_rows)])
        chosen = wanted[ordering]
        return (wide_index + chosen - REACH + N_WIDE) % N_WIDE
    owners = jax.vmap(one_device)(jax.random.split(key_rows, devices), wide_of)
    local_block = jax.random.randint(key_place, (devices, P_DEV), 0, TB_DEV)
    return (owners * TB_DEV + local_block).reshape(devices * P_DEV).astype(jnp.int32)


def draw_pair_count(key, part):
    key = jax.random.fold_in(key, 303)
    devices = N_WIDE * N_NARROW
    key_counts, key_full = jax.random.split(key)
    counts = jax.random.randint(key_counts, (devices,), P_DEV // 2, P_DEV + 1)
    fullest = jax.random.randint(key_full, (), 0, devices)
    return counts.at[fullest].set(P_DEV).astype(jnp.int32)


def with_ends(result, stream_key, low, high):
    dims = result.shape
    place = [jax.random.randint(jax.random.fold_in(stream_key, axis), (), 0, dims[axis]) for axis in range(len(dims))]
    result = result.at[tuple(place)].set(low)
    longest = dims.index(max(dims))
    place[longest] = (place[longest] + 1) % dims[longest]
    return result.at[tuple(place)].set(high)


def shard_levels(key, extent, cuts, smallest, high):
    def one(position, blocks):
        heights = jax.random.uniform(jax.random.fold_in(jax.random.fold_in(key, 6), position), (blocks,), jnp.float32, smallest / len(cuts), high / len(cuts))
        return jnp.repeat(jnp.exp(heights), extent[position] // blocks).reshape((-1,) + (1,) * (len(extent) - position - 1))

    loudness = one(*cuts[0])
    for cut in cuts[1:]:
        loudness = loudness * one(*cut)
    return loudness


def noise(stream_key, dims, width, most, cuts=(), kind=jnp.bfloat16):
    level = shard_levels(stream_key, dims, cuts, -0.22, 0.18) if cuts else 1.0
    drawn = jax.random.normal(stream_key, dims, jnp.float32) * width * level
    return jnp.minimum(jnp.maximum(drawn, -most), most).astype(kind)


def setup_inputs(seed: int = 0) -> dict:
    streams_of = jax.random.split(jax.random.key(seed), 7)
    src_field = noise(streams_of[0], (VARS, LEV, SRC_CELLS), 1.0, 6.0, ((1, 2), (2, 16)))
    src_depth = draw_src_depth(jax.random.fold_in(streams_of[6], 71), 0)
    packed_counts = draw_packed_counts(jax.random.fold_in(streams_of[6], 71), 0)
    pair_source = with_ends(jax.random.randint(streams_of[3], (PAIRS,), 0, SB_DEV), jax.random.fold_in(streams_of[3], 1), 0, SB_DEV - 1).astype(jnp.int32)
    pair_home = draw_pair_home(jax.random.fold_in(streams_of[6], 71), 0)
    pair_count = draw_pair_count(jax.random.fold_in(streams_of[6], 71), 0)
    return dict(src_field=src_field, src_depth=src_depth, packed_counts=packed_counts, pair_source=pair_source, pair_home=pair_home, pair_count=pair_count)


wet_limit = 1e-3


def unpack_counts(packed_words):
    lower_half = packed_words % 65536
    upper_half = packed_words // 65536
    return jnp.concatenate([lower_half, upper_half], axis=-2)


def stack_cells(field_block, depth_cells):
    level_ids = jnp.arange(field_block.shape[1], dtype=jnp.int32)
    wet_levels = level_ids[:, None] < depth_cells[None, :]
    masked = jnp.where(wet_levels[None, :, :], field_block, jnp.zeros_like(field_block))
    wet_ones = wet_levels.astype(field_block.dtype)
    return jnp.concatenate([jnp.transpose(masked, (1, 0, 2)), wet_ones[:, None, :]], axis=1)


def reference(src_field, src_depth, packed_counts, pair_source, pair_home, pair_count):
    device_total = pair_count.shape[0]
    own_cells = SB_DEV * BLK
    components = VARS + 1
    block_total = jnp.zeros((TB_DEV * N_WIDE, LEV, components, BLK), jnp.float32)

    def add_device(device_index, running):
        device_index = device_index.astype(jnp.int32)
        device_field = lax.dynamic_slice_in_dim(src_field, device_index * own_cells, own_cells, 2)
        cell_depth = lax.dynamic_slice_in_dim(src_depth, device_index * own_cells, own_cells, 0)
        device_packed = lax.dynamic_slice_in_dim(packed_counts, device_index * P_DEV, P_DEV, 0)
        source = lax.dynamic_slice_in_dim(pair_source, device_index * P_DEV, P_DEV, 0)
        home_block = lax.dynamic_slice_in_dim(pair_home, device_index * P_DEV, P_DEV, 0)
        live_count = lax.dynamic_slice_in_dim(pair_count, device_index, 1, 0)[0]
        stacked = stack_cells(device_field, cell_depth).reshape(LEV, components, SB_DEV, BLK)
        picked = jnp.take(stacked, source, axis=2)
        weight = (unpack_counts(device_packed).astype(jnp.float32) / DENOM).astype(jnp.bfloat16)
        pair_terms = jnp.einsum("pts,lcps->plct", weight.astype(jnp.float32), picked.astype(jnp.float32))
        pair_terms = lax.optimization_barrier(pair_terms.astype(jnp.bfloat16)).astype(jnp.float32)
        is_live = jnp.arange(P_DEV, dtype=jnp.int32) < live_count
        pair_terms = jnp.where(is_live[:, None, None, None], pair_terms, jnp.zeros_like(pair_terms))
        return running.at[home_block].add(pair_terms)

    block_total = lax.fori_loop(0, device_total, add_device, block_total)
    numerators = block_total[:, :, :VARS, :]
    wet_total = block_total[:, :, VARS, :]
    covered = wet_total > wet_limit
    safe_wet = jnp.where(covered, wet_total, jnp.ones_like(wet_total))
    remapped = jnp.where(covered[:, :, None, :], numerators / safe_wet[:, :, None, :], jnp.zeros_like(numerators))
    remapped = jnp.transpose(remapped, (2, 1, 0, 3)).reshape(VARS, LEV, TB_DEV * N_WIDE * BLK)
    return remapped.astype(jnp.bfloat16)
```

```python
import functools

import jax
import jax.numpy as jnp
from jax import lax
from jax.experimental import pallas as pl
from jax.experimental.pallas import tpu as pltpu
from jax.sharding import PartitionSpec as P

DENOM = 256
TB_DEV = 64
REGIONS = 5

wet_limit = 0.001


def round_up(value, multiple):
    return -(-value // multiple) * multiple


def sum_kernel(
    source_ref, slot_ref, base_ref, packed_ref, *rest, groups, part_levels, rows, in_kernel
):
    if in_kernel:
        pieces = rest[:groups]
        depth_ref = rest[groups]
        rest = rest[groups + 1 :]
        outs = rest[: 4 * groups]
        acc_ref, stack_ref = rest[4 * groups :]
    else:
        stack_ref = rest[0]
        outs = rest[1 : 1 + 4 * groups]
        acc_ref = rest[1 + 4 * groups]
    step = pl.program_id(0)
    per_step = packed_ref.shape[0]

    @pl.when(step == 0)
    def _():
        acc_ref[...] = jnp.zeros_like(acc_ref)
        if in_kernel:
            tiles = stack_ref.shape[0]
            for tile in range(tiles):
                cut = pl.ds(tile * 128, 128)
                depth = depth_ref[:, cut]
                parts = []
                for k in range(groups):
                    level = base_ref[k] + lax.broadcasted_iota(jnp.int32, (part_levels, 128), 0)
                    wet = level < depth
                    for v in range(pieces[k].shape[0]):
                        cells = pieces[k][v, :, cut].astype(jnp.float32)
                        parts.append(jnp.where(wet, cells, 0.0))
                    parts.append(jnp.where(wet, 1.0, 0.0))
                stack_ref[tile] = jnp.concatenate(parts, axis=0).astype(jnp.bfloat16)

    for q in range(per_step):
        pair = step * per_step + q
        words = packed_ref[q]
        low = (words & 65535).astype(jnp.float32)
        high = (words >> 16).astype(jnp.float32)
        weight = (jnp.concatenate([low, high], axis=0) * (1.0 / DENOM)).astype(jnp.bfloat16)
        term = lax.dot_general(
            stack_ref[source_ref[pair]],
            weight,
            (((1,), (1,)), ((), ())),
            preferred_element_type=jnp.float32,
        )
        acc_ref[slot_ref[pair]] += term

    @pl.when(step == pl.num_programs(0) - 1)
    def _():
        for k in range(groups):
            cut = slice(k * rows, (k + 1) * rows)
            for o, (first, last) in enumerate(((0, 2), (2, 3), (3, 4), (4, 5))):
                value = acc_ref[first * TB_DEV : last * TB_DEV, cut, :]
                out = outs[4 * k + o]
                out[...] = value.reshape(out.shape).astype(out.dtype)


def pair_sums(source, slot, base, packed, cells, groups, part_levels, rows, in_kernel):
    slots, half, block = packed.shape
    per_step = 16 if slots % 16 == 0 else 1
    whole = lambda a: pl.BlockSpec(a.shape, lambda i, *_: (0,) * a.ndim)
    regions = (2, 1, 1, 1)
    shapes = [
        jax.ShapeDtypeStruct((r * TB_DEV * rows, block), jnp.bfloat16)
        for _ in range(groups)
        for r in regions
    ]
    scratch = [pltpu.VMEM((REGIONS * TB_DEV + 1, groups * rows, block), jnp.float32)]
    if in_kernel:
        tiles = cells[-1].shape[1] // block
        scratch.append(pltpu.VMEM((tiles, groups * rows, block), jnp.bfloat16))
    return pl.pallas_call(
        functools.partial(
            sum_kernel, groups=groups, part_levels=part_levels, rows=rows, in_kernel=in_kernel
        ),
        out_shape=shapes,
        grid_spec=pltpu.PrefetchScalarGridSpec(
            num_scalar_prefetch=3,
            grid=(slots // per_step,),
            in_specs=[pl.BlockSpec((per_step, half, block), lambda i, *_: (i, 0, 0))]
            + [whole(c) for c in cells],
            out_specs=[whole(s) for s in shapes],
            scratch_shapes=scratch,
        ),
        compiler_params=pltpu.CompilerParams(dimension_semantics=("arbitrary",)),
        name="pair_sums",
    )(source, slot, base, packed, *cells)


def divide_kernel(*refs, part_levels, field_vars):
    out_ref = refs[-1]
    rows = (field_vars + 1) * part_levels

    for b in range(TB_DEV):
        cut = slice(b * rows, (b + 1) * rows)
        total = refs[0][cut, :].astype(jnp.float32)
        for ref in refs[1:-1]:
            total = total + ref[cut, :].astype(jnp.float32)
        wet = total[field_vars * part_levels :]
        covered = wet > wet_limit
        safe = jnp.where(covered, wet, 1.0)
        for v in range(field_vars):
            value = total[v * part_levels : (v + 1) * part_levels] / safe
            out_ref[v, :, b * 128 : (b + 1) * 128] = jnp.where(covered, value, 0.0).astype(
                out_ref.dtype
            )


def divided(parts, part_levels, field_vars, rows, in_kernel):
    block = parts[0].shape[1]
    shape = (field_vars, part_levels, TB_DEV * block)
    if in_kernel:
        return pl.pallas_call(
            functools.partial(divide_kernel, part_levels=part_levels, field_vars=field_vars),
            out_shape=jax.ShapeDtypeStruct(shape, jnp.bfloat16),
            name="divide",
        )(*parts)
    total = sum(p.astype(jnp.float32) for p in parts).reshape(TB_DEV, rows, block)
    total = total[:, : (field_vars + 1) * part_levels].reshape(TB_DEV, -1, part_levels, block)
    wet = total[:, field_vars:]
    covered = wet > wet_limit
    value = total[:, :field_vars] / jnp.where(covered, wet, 1.0)
    value = jnp.where(covered, value, 0.0)
    return jnp.transpose(value, (1, 2, 0, 3)).reshape(shape).astype(jnp.bfloat16)


def per_device(src_field, src_depth, packed_counts, pair_source, pair_home, pair_count):
    groups = lax.axis_size("narrow")
    wide_size = lax.axis_size("wide")
    field_vars, part_levels, _ = src_field.shape
    block = packed_counts.shape[2]
    own_cells = src_depth.shape[0]
    tiles = own_cells // block
    pair_slots = pair_source.shape[0]
    rows = round_up((field_vars + 1) * part_levels, 8)
    in_kernel = part_levels % 8 == 0 and block == 128
    narrow_index = lax.axis_index("narrow")
    wide_index = lax.axis_index("wide")

    pieces = []
    for k in range(groups):
        start = ((narrow_index + k) % groups) * own_cells
        piece = lax.dynamic_slice_in_dim(src_field, start, own_cells, 2)
        if k:
            piece = lax.ppermute(piece, "narrow", [(i, (i + k) % groups) for i in range(groups)])
        pieces.append(piece)
    steps = jnp.arange(groups, dtype=jnp.int32)
    base = ((narrow_index - steps + groups) % groups * part_levels).astype(jnp.int32)

    chips = wide_size // 2
    core, chip = wide_index % 2, wide_index // 2
    side = chip % 2
    target = pair_home // TB_DEV
    step = (target // 2 - chip + 1 + chips) % chips - 1
    across = jnp.where(side == 0, 1, -1)
    same_core = target % 2 == core
    region = jnp.where(
        same_core,
        jnp.where(step == 0, 4, jnp.where(step == across, 3, 2)),
        jnp.where(step == 0, 0, 1),
    )
    live = jnp.arange(pair_slots, dtype=jnp.int32) < pair_count[0]
    slot = jnp.where(live, region * TB_DEV + pair_home % TB_DEV, REGIONS * TB_DEV)
    slot = slot.astype(jnp.int32)

    if in_kernel:
        cells = pieces + [src_depth.reshape(1, own_cells)]
    else:
        stack = []
        for k in range(groups):
            level = base[k] + jnp.arange(part_levels, dtype=jnp.int32)
            wet = level[:, None] < src_depth[None, :]
            masked = jnp.where(wet[None], pieces[k], jnp.zeros_like(pieces[k]))
            both = jnp.concatenate([masked, wet[None].astype(jnp.bfloat16)], axis=0)
            both = both.reshape(-1, own_cells)
            stack.append(jnp.pad(both, ((0, rows - both.shape[0]), (0, 0))))
        stack = jnp.concatenate(stack, axis=0).reshape(groups * rows, tiles, block)
        cells = [jnp.transpose(stack, (1, 0, 2))]
    sums = pair_sums(
        pair_source, slot, base, packed_counts, cells, groups, part_levels, rows, in_kernel
    )

    to_core = [(w, w ^ 1) for w in range(wide_size)]
    to_column = [(w, (w + (4 if w // 2 % 2 else -4)) % wide_size) for w in range(wide_size)]
    to_side = [(w, w ^ 2) for w in range(wide_size)]
    for_column = core != side
    unit = TB_DEV * rows
    zero = jnp.zeros((), jnp.float32)
    wider = lambda a: a.astype(jnp.float32)
    final = []
    for k in list(range(1, groups)) + [0]:
        out_core, own_column, own_side, own_home = sums[4 * k : 4 * k + 4]
        from_core = lax.ppermute(out_core, "wide", to_core)
        partner_home, partner_away = from_core[:unit], wider(from_core[unit:])
        column = wider(own_column) + jnp.where(for_column, partner_away, zero)
        from_column = lax.ppermute(column.astype(jnp.bfloat16), "wide", to_column)
        side_sum = wider(own_side) + jnp.where(for_column, zero, partner_away)
        side_sum = side_sum + wider(from_column)
        from_side = lax.ppermute(side_sum.astype(jnp.bfloat16), "wide", to_side)
        if k:
            total = wider(own_home) + wider(partner_home) + wider(from_side)
            route = [(i, (i - k) % groups) for i in range(groups)]
            final.append(lax.ppermute(total.astype(jnp.bfloat16), "narrow", route))
        else:
            final += [own_home, partner_home, from_side]
    return divided(final, part_levels, field_vars, rows, in_kernel)


def solution(mesh):
    placed = (
        P(None, "narrow", "wide"),
        P(("wide", "narrow")),
        P(("wide", "narrow"), None, None),
        P(("wide", "narrow")),
        P(("wide", "narrow")),
        P(("wide", "narrow")),
    )
    return jax.shard_map(
        per_device, mesh=mesh, in_specs=placed, out_specs=P(None, "narrow", "wide"), check_vma=False
    )
```

```python
import functools

import jax
import jax.numpy as jnp
from jax import lax
from jax.experimental import pallas as pl
from jax.experimental.pallas import tpu as pltpu
from jax.sharding import PartitionSpec as P

DENOM = 256
TB_DEV = 64
REGIONS = 5
FIRST_PART = 36

wet_limit = 0.001


def round_up(value, multiple):
    return -(-value // multiple) * multiple


def sum_kernel(
    source_ref, slot_ref, base_ref, packed_ref, *rest, groups, part_levels, rows, in_kernel
):
    if in_kernel:
        pieces = rest[:groups]
        depth_ref = rest[groups]
        rest = rest[groups + 1 :]
        outs = rest[: 4 * groups]
        acc_ref, stack_ref = rest[4 * groups :]
    else:
        stack_ref = rest[0]
        outs = rest[1 : 1 + 4 * groups]
        acc_ref = rest[1 + 4 * groups]
    step = pl.program_id(0)
    per_step = packed_ref.shape[0]

    @pl.when(step == 0)
    def _():
        acc_ref[...] = jnp.zeros_like(acc_ref)
        if in_kernel:
            tiles = stack_ref.shape[0]
            for tile in range(tiles):
                cut = pl.ds(tile * 128, 128)
                depth = depth_ref[:, cut]
                parts = []
                for k in range(groups):
                    level = base_ref[k] + lax.broadcasted_iota(jnp.int32, (part_levels, 128), 0)
                    wet = level < depth
                    for v in range(pieces[k].shape[0]):
                        cells = pieces[k][v, :, cut].astype(jnp.float32)
                        parts.append(jnp.where(wet, cells, 0.0))
                    parts.append(jnp.where(wet, 1.0, 0.0))
                stack_ref[tile] = jnp.concatenate(parts, axis=0).astype(jnp.bfloat16)

    for q in range(per_step):
        pair = step * per_step + q
        words = packed_ref[q]
        low = (words & 65535).astype(jnp.float32)
        high = (words >> 16).astype(jnp.float32)
        weight = (jnp.concatenate([low, high], axis=0) * (1.0 / DENOM)).astype(jnp.bfloat16)
        term = lax.dot_general(
            stack_ref[source_ref[pair]],
            weight,
            (((1,), (1,)), ((), ())),
            preferred_element_type=jnp.float32,
        )
        acc_ref[slot_ref[pair]] += term

    @pl.when(step == pl.num_programs(0) - 1)
    def _():
        for k in range(groups):
            cut = slice(k * rows, (k + 1) * rows)
            for o, (first, last) in enumerate(((0, 2), (2, 3), (3, 4), (4, 5))):
                value = acc_ref[first * TB_DEV : last * TB_DEV, cut, :]
                out = outs[4 * k + o]
                out[...] = value.reshape(out.shape).astype(out.dtype)


def pair_sums(source, slot, base, packed, cells, groups, part_levels, rows, in_kernel):
    slots, half, block = packed.shape
    per_step = 16 if slots % 16 == 0 else 1
    whole = lambda a: pl.BlockSpec(a.shape, lambda i, *_: (0,) * a.ndim)
    regions = (2, 1, 1, 1)
    shapes = [
        jax.ShapeDtypeStruct((r * TB_DEV * rows, block), jnp.bfloat16)
        for _ in range(groups)
        for r in regions
    ]
    scratch = [pltpu.VMEM((REGIONS * TB_DEV + 1, groups * rows, block), jnp.float32)]
    if in_kernel:
        tiles = cells[-1].shape[1] // block
        scratch.append(pltpu.VMEM((tiles, groups * rows, block), jnp.bfloat16))
    return pl.pallas_call(
        functools.partial(
            sum_kernel, groups=groups, part_levels=part_levels, rows=rows, in_kernel=in_kernel
        ),
        out_shape=shapes,
        grid_spec=pltpu.PrefetchScalarGridSpec(
            num_scalar_prefetch=3,
            grid=(slots // per_step,),
            in_specs=[pl.BlockSpec((per_step, half, block), lambda i, *_: (i, 0, 0))]
            + [whole(c) for c in cells],
            out_specs=[whole(s) for s in shapes],
            scratch_shapes=scratch,
        ),
        compiler_params=pltpu.CompilerParams(dimension_semantics=("arbitrary",)),
        name="pair_sums",
    )(source, slot, base, packed, *cells)


def divide_kernel(*refs, part_levels, field_vars):
    out_ref = refs[-1]
    rows = (field_vars + 1) * part_levels

    for b in range(TB_DEV):
        cut = slice(b * rows, (b + 1) * rows)
        part, place = (0, b) if b < FIRST_PART else (1, b - FIRST_PART)
        total = refs[part][place * rows : (place + 1) * rows, :].astype(jnp.float32)
        for ref in refs[2:-1]:
            total = total + ref[cut, :].astype(jnp.float32)
        wet = total[field_vars * part_levels :]
        covered = wet > wet_limit
        safe = jnp.where(covered, wet, 1.0)
        for v in range(field_vars):
            value = total[v * part_levels : (v + 1) * part_levels] / safe
            out_ref[v, :, b * 128 : (b + 1) * 128] = jnp.where(covered, value, 0.0).astype(
                out_ref.dtype
            )


def divided(parts, halves, part_levels, field_vars, rows, in_kernel):
    block = parts[0].shape[1]
    unit = TB_DEV * rows
    shape = (field_vars, part_levels, TB_DEV * block)
    if in_kernel:
        return pl.pallas_call(
            functools.partial(divide_kernel, part_levels=part_levels, field_vars=field_vars),
            out_shape=jax.ShapeDtypeStruct(shape, jnp.bfloat16),
            name="divide",
        )(*halves, *parts)
    parts = [p[:unit] for p in parts] + [jnp.concatenate(halves, axis=0)]
    total = sum(p.astype(jnp.float32) for p in parts).reshape(TB_DEV, rows, block)
    total = total[:, : (field_vars + 1) * part_levels].reshape(TB_DEV, -1, part_levels, block)
    wet = total[:, field_vars:]
    covered = wet > wet_limit
    value = total[:, :field_vars] / jnp.where(covered, wet, 1.0)
    value = jnp.where(covered, value, 0.0)
    return jnp.transpose(value, (1, 2, 0, 3)).reshape(shape).astype(jnp.bfloat16)


def per_device(src_field, src_depth, packed_counts, pair_source, pair_home, pair_count):
    groups = lax.axis_size("narrow")
    wide_size = lax.axis_size("wide")
    field_vars, part_levels, _ = src_field.shape
    block = packed_counts.shape[2]
    own_cells = src_depth.shape[0]
    tiles = own_cells // block
    pair_slots = pair_source.shape[0]
    rows = round_up((field_vars + 1) * part_levels, 8)
    in_kernel = part_levels % 8 == 0 and block == 128
    narrow_index = lax.axis_index("narrow")
    wide_index = lax.axis_index("wide")

    pieces = []
    for k in range(groups):
        start = ((narrow_index + k) % groups) * own_cells
        piece = lax.dynamic_slice_in_dim(src_field, start, own_cells, 2)
        if k:
            piece = lax.ppermute(piece, "narrow", [(i, (i + k) % groups) for i in range(groups)])
        pieces.append(piece)
    steps = jnp.arange(groups, dtype=jnp.int32)
    base = ((narrow_index - steps + groups) % groups * part_levels).astype(jnp.int32)

    chips = wide_size // 2
    core, chip = wide_index % 2, wide_index // 2
    side = chip % 2
    target = pair_home // TB_DEV
    step = (target // 2 - chip + 1 + chips) % chips - 1
    across = jnp.where(side == 0, 1, -1)
    same_core = target % 2 == core
    region = jnp.where(
        same_core,
        jnp.where(step == 0, 4, jnp.where(step == across, 3, 2)),
        jnp.where(step == 0, 0, 1),
    )
    live = jnp.arange(pair_slots, dtype=jnp.int32) < pair_count[0]
    slot = jnp.where(live, region * TB_DEV + pair_home % TB_DEV, REGIONS * TB_DEV)
    slot = slot.astype(jnp.int32)

    if in_kernel:
        cells = pieces + [src_depth.reshape(1, own_cells)]
    else:
        stack = []
        for k in range(groups):
            level = base[k] + jnp.arange(part_levels, dtype=jnp.int32)
            wet = level[:, None] < src_depth[None, :]
            masked = jnp.where(wet[None], pieces[k], jnp.zeros_like(pieces[k]))
            both = jnp.concatenate([masked, wet[None].astype(jnp.bfloat16)], axis=0)
            both = both.reshape(-1, own_cells)
            stack.append(jnp.pad(both, ((0, rows - both.shape[0]), (0, 0))))
        stack = jnp.concatenate(stack, axis=0).reshape(groups * rows, tiles, block)
        cells = [jnp.transpose(stack, (1, 0, 2))]
    sums = pair_sums(
        pair_source, slot, base, packed_counts, cells, groups, part_levels, rows, in_kernel
    )

    to_core = [(w, w ^ 1) for w in range(wide_size)]
    to_column = [(w, (w + (4 if w // 2 % 2 else -4)) % wide_size) for w in range(wide_size)]
    to_side = [(w, w ^ 2) for w in range(wide_size)]
    for_column = core != side
    unit = TB_DEV * rows
    zero = jnp.zeros((), jnp.float32)
    wider = lambda a: a.astype(jnp.float32)
    narrower = lambda a: a.astype(jnp.bfloat16)
    back = [[(i, (i - k) % groups) for i in range(groups)] for k in range(groups)]
    first = FIRST_PART * rows
    halves = [slice(0, first), slice(first, unit)]
    from_core = [lax.ppermute(sums[4 * k], "wide", to_core) for k in range(groups)]

    def column_part(k, half):
        away = wider(from_core[k][unit:][half])
        return wider(sums[4 * k + 1][half]) + jnp.where(for_column, away, zero)

    def side_part(k, half):
        away = wider(from_core[k][unit:][half])
        return wider(sums[4 * k + 2][half]) + jnp.where(for_column, zero, away)

    column_sent = [
        [lax.ppermute(narrower(column_part(k, half)), "narrow", back[k]) for k in range(1, groups)]
        for half in halves
    ]
    other_side = [
        lax.ppermute(narrower(side_part(k, slice(0, unit))), "wide", to_side)
        for k in range(1, groups)
    ]
    from_column = []
    for half, received in zip(halves, column_sent):
        column = column_part(0, half)
        for piece in received:
            column = column + wider(piece)
        from_column.append(lax.ppermute(narrower(column), "wide", to_column))
    from_narrow = []
    for k in range(1, groups):
        total = wider(sums[4 * k + 3]) + wider(from_core[k][:unit]) + wider(other_side[k - 1])
        from_narrow.append(lax.ppermute(narrower(total), "narrow", back[k]))
    from_side = [
        lax.ppermute(narrower(side_part(0, half) + wider(piece)), "wide", to_side)
        for half, piece in zip(halves, from_column)
    ]
    final = [sums[3], from_core[0]] + from_narrow
    return divided(final, from_side, part_levels, field_vars, rows, in_kernel)


def solution(mesh):
    placed = (
        P(None, "narrow", "wide"),
        P(("wide", "narrow")),
        P(("wide", "narrow"), None, None),
        P(("wide", "narrow")),
        P(("wide", "narrow")),
        P(("wide", "narrow")),
    )
    return jax.shard_map(
        per_device, mesh=mesh, in_specs=placed, out_specs=P(None, "narrow", "wide"), check_vma=False
    )
```

```python
import functools

import jax
import jax.numpy as jnp
from jax import lax
from jax.experimental import pallas as pl
from jax.experimental.pallas import tpu as pltpu
from jax.sharding import PartitionSpec as P

DENOM = 256
TB_DEV = 64
REGIONS = 5
FIRST_PART = 36

wet_limit = 0.001


def round_up(value, multiple):
    return -(-value // multiple) * multiple


def sum_kernel(
    source_ref, slot_ref, base_ref, packed_ref, *rest, groups, part_levels, rows, in_kernel
):
    if in_kernel:
        pieces = rest[:groups]
        depth_ref = rest[groups]
        rest = rest[groups + 1 :]
        outs = rest[: 4 * groups]
        acc_ref, stack_ref = rest[4 * groups :]
    else:
        stack_ref = rest[0]
        outs = rest[1 : 1 + 4 * groups]
        acc_ref = rest[1 + 4 * groups]
    step = pl.program_id(0)
    per_step = packed_ref.shape[0]

    @pl.when(step == 0)
    def _():
        acc_ref[...] = jnp.zeros_like(acc_ref)
        if in_kernel:
            tiles = stack_ref.shape[0]
            for tile in range(tiles):
                cut = pl.ds(tile * 128, 128)
                depth = depth_ref[:, cut]
                parts = []
                for k in range(groups):
                    level = base_ref[k] + lax.broadcasted_iota(jnp.int32, (part_levels, 128), 0)
                    wet = level < depth
                    for v in range(pieces[k].shape[0]):
                        cells = pieces[k][v, :, cut].astype(jnp.float32)
                        parts.append(jnp.where(wet, cells, 0.0))
                    parts.append(jnp.where(wet, 1.0, 0.0))
                stack_ref[tile] = jnp.concatenate(parts, axis=0).astype(jnp.bfloat16)

    for q in range(per_step):
        pair = step * per_step + q
        words = packed_ref[q]
        low = (words & 65535).astype(jnp.float32)
        high = (words >> 16).astype(jnp.float32)
        weight = (jnp.concatenate([low, high], axis=0) * (1.0 / DENOM)).astype(jnp.bfloat16)
        term = lax.dot_general(
            stack_ref[source_ref[pair]],
            weight,
            (((1,), (1,)), ((), ())),
            preferred_element_type=jnp.float32,
        )
        acc_ref[slot_ref[pair]] += term

    @pl.when(step == pl.num_programs(0) - 1)
    def _():
        for k in range(groups):
            cut = slice(k * rows, (k + 1) * rows)
            for o, (first, last) in enumerate(((0, 2), (2, 3), (3, 4), (4, 5))):
                value = acc_ref[first * TB_DEV : last * TB_DEV, cut, :]
                out = outs[4 * k + o]
                out[...] = value.reshape(out.shape).astype(out.dtype)


def pair_sums(source, slot, base, packed, cells, groups, part_levels, rows, in_kernel):
    slots, half, block = packed.shape
    per_step = 16 if slots % 16 == 0 else 1
    whole = lambda a: pl.BlockSpec(a.shape, lambda i, *_: (0,) * a.ndim)
    regions = (2, 1, 1, 1)
    shapes = [
        pltpu.VMEM((r * TB_DEV * rows, block), jnp.bfloat16)
        for _ in range(groups)
        for r in regions
    ]
    scratch = [pltpu.VMEM((REGIONS * TB_DEV + 1, groups * rows, block), jnp.float32)]
    if in_kernel:
        tiles = cells[-1].shape[1] // block
        scratch.append(pltpu.VMEM((tiles, groups * rows, block), jnp.bfloat16))
    return pl.pallas_call(
        functools.partial(
            sum_kernel, groups=groups, part_levels=part_levels, rows=rows, in_kernel=in_kernel
        ),
        out_shape=shapes,
        grid_spec=pltpu.PrefetchScalarGridSpec(
            num_scalar_prefetch=3,
            grid=(slots // per_step,),
            in_specs=[pl.BlockSpec((per_step, half, block), lambda i, *_: (i, 0, 0))]
            + [whole(c) for c in cells],
            out_specs=[pl.BlockSpec(memory_space=pltpu.VMEM)] * len(shapes),
            scratch_shapes=scratch,
        ),
        compiler_params=pltpu.CompilerParams(dimension_semantics=("arbitrary",), vmem_limit_bytes=28 << 20),
        name="pair_sums",
    )(source, slot, base, packed, *cells)


def divide_kernel(*refs, part_levels, field_vars):
    out_ref = refs[-1]
    rows = (field_vars + 1) * part_levels

    for b in range(TB_DEV):
        cut = slice(b * rows, (b + 1) * rows)
        part, place = (0, b) if b < FIRST_PART else (1, b - FIRST_PART)
        total = refs[part][place * rows : (place + 1) * rows, :].astype(jnp.float32)
        for ref in refs[2:-1]:
            total = total + ref[cut, :].astype(jnp.float32)
        wet = total[field_vars * part_levels :]
        covered = wet > wet_limit
        safe = jnp.where(covered, wet, 1.0)
        for v in range(field_vars):
            value = total[v * part_levels : (v + 1) * part_levels] / safe
            out_ref[v, :, b * 128 : (b + 1) * 128] = jnp.where(covered, value, 0.0).astype(
                out_ref.dtype
            )


def divided(parts, halves, part_levels, field_vars, rows, in_kernel):
    block = parts[0].shape[1]
    unit = TB_DEV * rows
    shape = (field_vars, part_levels, TB_DEV * block)
    if in_kernel:
        return pl.pallas_call(
            functools.partial(divide_kernel, part_levels=part_levels, field_vars=field_vars),
            out_shape=jax.ShapeDtypeStruct(shape, jnp.bfloat16),
            name="divide",
        )(*halves, *parts)
    parts = [p[:unit] for p in parts] + [jnp.concatenate(halves, axis=0)]
    total = sum(p.astype(jnp.float32) for p in parts).reshape(TB_DEV, rows, block)
    total = total[:, : (field_vars + 1) * part_levels].reshape(TB_DEV, -1, part_levels, block)
    wet = total[:, field_vars:]
    covered = wet > wet_limit
    value = total[:, :field_vars] / jnp.where(covered, wet, 1.0)
    value = jnp.where(covered, value, 0.0)
    return jnp.transpose(value, (1, 2, 0, 3)).reshape(shape).astype(jnp.bfloat16)


def per_device(src_field, src_depth, packed_counts, pair_source, pair_home, pair_count):
    groups = lax.axis_size("narrow")
    wide_size = lax.axis_size("wide")
    field_vars, part_levels, _ = src_field.shape
    block = packed_counts.shape[2]
    own_cells = src_depth.shape[0]
    tiles = own_cells // block
    pair_slots = pair_source.shape[0]
    rows = round_up((field_vars + 1) * part_levels, 8)
    in_kernel = part_levels % 8 == 0 and block == 128
    narrow_index = lax.axis_index("narrow")
    wide_index = lax.axis_index("wide")

    pieces = []
    for k in range(groups):
        start = ((narrow_index + k) % groups) * own_cells
        piece = lax.dynamic_slice_in_dim(src_field, start, own_cells, 2)
        if k:
            piece = lax.ppermute(piece, "narrow", [(i, (i + k) % groups) for i in range(groups)])
        pieces.append(piece)
    steps = jnp.arange(groups, dtype=jnp.int32)
    base = ((narrow_index - steps + groups) % groups * part_levels).astype(jnp.int32)

    chips = wide_size // 2
    core, chip = wide_index % 2, wide_index // 2
    side = chip % 2
    target = pair_home // TB_DEV
    step = (target // 2 - chip + 1 + chips) % chips - 1
    across = jnp.where(side == 0, 1, -1)
    same_core = target % 2 == core
    region = jnp.where(
        same_core,
        jnp.where(step == 0, 4, jnp.where(step == across, 3, 2)),
        jnp.where(step == 0, 0, 1),
    )
    live = jnp.arange(pair_slots, dtype=jnp.int32) < pair_count[0]
    slot = jnp.where(live, region * TB_DEV + pair_home % TB_DEV, REGIONS * TB_DEV)
    slot = slot.astype(jnp.int32)

    if in_kernel:
        cells = pieces + [src_depth.reshape(1, own_cells)]
    else:
        stack = []
        for k in range(groups):
            level = base[k] + jnp.arange(part_levels, dtype=jnp.int32)
            wet = level[:, None] < src_depth[None, :]
            masked = jnp.where(wet[None], pieces[k], jnp.zeros_like(pieces[k]))
            both = jnp.concatenate([masked, wet[None].astype(jnp.bfloat16)], axis=0)
            both = both.reshape(-1, own_cells)
            stack.append(jnp.pad(both, ((0, rows - both.shape[0]), (0, 0))))
        stack = jnp.concatenate(stack, axis=0).reshape(groups * rows, tiles, block)
        cells = [jnp.transpose(stack, (1, 0, 2))]
    sums = pair_sums(
        pair_source, slot, base, packed_counts, cells, groups, part_levels, rows, in_kernel
    )

    to_core = [(w, w ^ 1) for w in range(wide_size)]
    to_column = [(w, (w + (4 if w // 2 % 2 else -4)) % wide_size) for w in range(wide_size)]
    to_side = [(w, w ^ 2) for w in range(wide_size)]
    for_column = core != side
    unit = TB_DEV * rows
    zero = jnp.zeros((), jnp.float32)
    wider = lambda a: a.astype(jnp.float32)
    narrower = lambda a: a.astype(jnp.bfloat16)
    back = [[(i, (i - k) % groups) for i in range(groups)] for k in range(groups)]
    first = FIRST_PART * rows
    halves = [slice(0, first), slice(first, unit)]
    from_core = [lax.ppermute(sums[4 * k], "wide", to_core) for k in range(groups)]

    def column_part(k, half):
        away = wider(from_core[k][unit:][half])
        return wider(sums[4 * k + 1][half]) + jnp.where(for_column, away, zero)

    def side_part(k, half):
        away = wider(from_core[k][unit:][half])
        return wider(sums[4 * k + 2][half]) + jnp.where(for_column, zero, away)

    column_sent = [
        [lax.ppermute(narrower(column_part(k, half)), "narrow", back[k]) for k in range(1, groups)]
        for half in halves
    ]
    other_side = [
        lax.ppermute(narrower(side_part(k, slice(0, unit))), "wide", to_side)
        for k in range(1, groups)
    ]
    from_column = []
    for half, received in zip(halves, column_sent):
        column = column_part(0, half)
        for piece in received:
            column = column + wider(piece)
        from_column.append(lax.ppermute(narrower(column), "wide", to_column))
    from_narrow = []
    for k in range(1, groups):
        total = wider(sums[4 * k + 3]) + wider(from_core[k][:unit]) + wider(other_side[k - 1])
        from_narrow.append(lax.ppermute(narrower(total), "narrow", back[k]))
    from_side = [
        lax.ppermute(narrower(side_part(0, half) + wider(piece)), "wide", to_side)
        for half, piece in zip(halves, from_column)
    ]
    final = [sums[3], from_core[0]] + from_narrow
    return divided(final, from_side, part_levels, field_vars, rows, in_kernel)


def solution(mesh):
    placed = (
        P(None, "narrow", "wide"),
        P(("wide", "narrow")),
        P(("wide", "narrow"), None, None),
        P(("wide", "narrow")),
        P(("wide", "narrow")),
        P(("wide", "narrow")),
    )
    return jax.shard_map(
        per_device, mesh=mesh, in_specs=placed, out_specs=P(None, "narrow", "wide"), check_vma=False
    )
```

```python
import functools

import jax
import jax.numpy as jnp
from jax import lax
from jax.experimental import pallas as pl
from jax.experimental.pallas import tpu as pltpu
from jax.sharding import PartitionSpec as P


DENOM = 256
TB_DEV = 64
REGIONS = 5
FIRST_PART = 36

wet_limit = 0.001


def round_up(value, multiple):
    return -(-value // multiple) * multiple


def sum_kernel(
    source_ref, slot_ref, base_ref, packed_ref, *rest, groups, part_levels, rows, in_kernel
):
    if in_kernel:
        pieces = rest[:groups]
        depth_ref = rest[groups]
        rest = rest[groups + 1 :]
        outs = rest[: 4 * groups]
        acc_ref, stack_ref = rest[4 * groups :]
    else:
        stack_ref = rest[0]
        outs = rest[1 : 1 + 4 * groups]
        acc_ref = rest[1 + 4 * groups]
    step = pl.program_id(0)
    per_step = packed_ref.shape[0]

    @pl.when(step == 0)
    def _():
        acc_ref[...] = jnp.zeros_like(acc_ref)
        if in_kernel:
            tiles = stack_ref.shape[0]
            for tile in range(tiles):
                cut = pl.ds(tile * 128, 128)
                depth = depth_ref[:, cut]
                parts = []
                for k in range(groups):
                    level = base_ref[k] + lax.broadcasted_iota(jnp.int32, (part_levels, 128), 0)
                    wet = level < depth
                    for v in range(pieces[k].shape[0]):
                        cells = pieces[k][v, :, cut].astype(jnp.float32)
                        parts.append(jnp.where(wet, cells, 0.0))
                    parts.append(jnp.where(wet, 1.0, 0.0))
                stack_ref[tile] = jnp.concatenate(parts, axis=0).astype(jnp.bfloat16)

    for q in range(per_step):
        pair = step * per_step + q
        words = packed_ref[q]
        low = (words & 65535).astype(jnp.float32)
        high = (words >> 16).astype(jnp.float32)
        weight = (jnp.concatenate([low, high], axis=0) * (1.0 / DENOM)).astype(jnp.bfloat16)
        term = lax.dot_general(
            stack_ref[source_ref[pair]],
            weight,
            (((1,), (1,)), ((), ())),
            preferred_element_type=jnp.float32,
        )
        acc_ref[slot_ref[pair]] += term

    @pl.when(step == pl.num_programs(0) - 1)
    def _():
        for k in range(groups):
            cut = slice(k * rows, (k + 1) * rows)
            for o, (first, last) in enumerate(((0, 2), (2, 3), (3, 4), (4, 5))):
                value = acc_ref[first * TB_DEV : last * TB_DEV, cut, :]
                out = outs[4 * k + o]
                out[...] = value.reshape(out.shape).astype(out.dtype)


def pair_sums(source, slot, base, packed, cells, groups, part_levels, rows, in_kernel):
    slots, half, block = packed.shape
    per_step = 16 if slots % 16 == 0 else 1
    whole = lambda a: pl.BlockSpec(a.shape, lambda i, *_: (0,) * a.ndim)
    regions = (2, 1, 1, 1)
    shapes = [
        pltpu.VMEM((r * TB_DEV * rows, block), jnp.bfloat16)
        for _ in range(groups)
        for r in regions
    ]
    scratch = [pltpu.VMEM((REGIONS * TB_DEV + 1, groups * rows, block), jnp.float32)]
    if in_kernel:
        tiles = cells[-1].shape[1] // block
        scratch.append(pltpu.VMEM((tiles, groups * rows, block), jnp.bfloat16))
    return pl.pallas_call(
        functools.partial(
            sum_kernel, groups=groups, part_levels=part_levels, rows=rows, in_kernel=in_kernel
        ),
        out_shape=shapes,
        grid_spec=pltpu.PrefetchScalarGridSpec(
            num_scalar_prefetch=3,
            grid=(slots // per_step,),
            in_specs=[pl.BlockSpec((per_step, half, block), lambda i, *_: (i, 0, 0))]
            + [whole(c) for c in cells],
            out_specs=[pl.BlockSpec(memory_space=pltpu.VMEM)] * len(shapes),
            scratch_shapes=scratch,
        ),
        compiler_params=pltpu.CompilerParams(dimension_semantics=("arbitrary",), vmem_limit_bytes=28 << 20),
        name="pair_sums",
    )(source, slot, base, packed, *cells)


def divide_kernel(*refs, part_levels, field_vars):
    out_ref = refs[-1]
    rows = (field_vars + 1) * part_levels

    for b in range(TB_DEV):
        cut = slice(b * rows, (b + 1) * rows)
        part, place = (0, b) if b < FIRST_PART else (1, b - FIRST_PART)
        total = refs[part][place * rows : (place + 1) * rows, :].astype(jnp.float32)
        for ref in refs[2:-1]:
            total = total + ref[cut, :].astype(jnp.float32)
        wet = total[field_vars * part_levels :]
        covered = wet > wet_limit
        safe = jnp.where(covered, wet, 1.0)
        for v in range(field_vars):
            value = total[v * part_levels : (v + 1) * part_levels] / safe
            out_ref[v, :, b * 128 : (b + 1) * 128] = jnp.where(covered, value, 0.0).astype(
                out_ref.dtype
            )


def divided(parts, halves, part_levels, field_vars, rows, in_kernel):
    block = parts[0].shape[1]
    unit = TB_DEV * rows
    shape = (field_vars, part_levels, TB_DEV * block)
    if in_kernel:
        return pl.pallas_call(
            functools.partial(divide_kernel, part_levels=part_levels, field_vars=field_vars),
            out_shape=jax.ShapeDtypeStruct(shape, jnp.bfloat16),
            compiler_params=pltpu.CompilerParams(vmem_limit_bytes=16 << 20),
            name="divide",
        )(*halves, *parts)
    parts = [p[:unit] for p in parts] + [jnp.concatenate(halves, axis=0)]
    total = sum(p.astype(jnp.float32) for p in parts).reshape(TB_DEV, rows, block)
    total = total[:, : (field_vars + 1) * part_levels].reshape(TB_DEV, -1, part_levels, block)
    wet = total[:, field_vars:]
    covered = wet > wet_limit
    value = total[:, :field_vars] / jnp.where(covered, wet, 1.0)
    value = jnp.where(covered, value, 0.0)
    return jnp.transpose(value, (1, 2, 0, 3)).reshape(shape).astype(jnp.bfloat16)


def per_device(src_field, src_depth, packed_counts, pair_source, pair_home, pair_count):
    groups = lax.axis_size("narrow")
    wide_size = lax.axis_size("wide")
    field_vars, part_levels, _ = src_field.shape
    block = packed_counts.shape[2]
    own_cells = src_depth.shape[0]
    tiles = own_cells // block
    pair_slots = pair_source.shape[0]
    rows = round_up((field_vars + 1) * part_levels, 8)
    in_kernel = part_levels % 8 == 0 and block == 128
    narrow_index = lax.axis_index("narrow")
    wide_index = lax.axis_index("wide")

    pieces = []
    for k in range(groups):
        start = ((narrow_index + k) % groups) * own_cells
        piece = lax.dynamic_slice_in_dim(src_field, start, own_cells, 2)
        if k:
            piece = lax.ppermute(piece, "narrow", [(i, (i + k) % groups) for i in range(groups)])
        pieces.append(piece)
    steps = jnp.arange(groups, dtype=jnp.int32)
    base = ((narrow_index - steps + groups) % groups * part_levels).astype(jnp.int32)

    chips = wide_size // 2
    core, chip = wide_index % 2, wide_index // 2
    side = chip % 2
    target = pair_home // TB_DEV
    step = (target // 2 - chip + 1 + chips) % chips - 1
    across = jnp.where(side == 0, 1, -1)
    same_core = target % 2 == core
    region = jnp.where(
        same_core,
        jnp.where(step == 0, 4, jnp.where(step == across, 3, 2)),
        jnp.where(step == 0, 0, 1),
    )
    live = jnp.arange(pair_slots, dtype=jnp.int32) < pair_count[0]
    slot = jnp.where(live, region * TB_DEV + pair_home % TB_DEV, REGIONS * TB_DEV)
    slot = slot.astype(jnp.int32)

    if in_kernel:
        cells = pieces + [src_depth.reshape(1, own_cells)]
    else:
        stack = []
        for k in range(groups):
            level = base[k] + jnp.arange(part_levels, dtype=jnp.int32)
            wet = level[:, None] < src_depth[None, :]
            masked = jnp.where(wet[None], pieces[k], jnp.zeros_like(pieces[k]))
            both = jnp.concatenate([masked, wet[None].astype(jnp.bfloat16)], axis=0)
            both = both.reshape(-1, own_cells)
            stack.append(jnp.pad(both, ((0, rows - both.shape[0]), (0, 0))))
        stack = jnp.concatenate(stack, axis=0).reshape(groups * rows, tiles, block)
        cells = [jnp.transpose(stack, (1, 0, 2))]
    sums = pair_sums(
        pair_source, slot, base, packed_counts, cells, groups, part_levels, rows, in_kernel
    )

    to_core = [(w, w ^ 1) for w in range(wide_size)]
    to_column = [(w, (w + (4 if w // 2 % 2 else -4)) % wide_size) for w in range(wide_size)]
    to_side = [(w, w ^ 2) for w in range(wide_size)]
    for_column = core != side
    unit = TB_DEV * rows
    zero = jnp.zeros((), jnp.float32)
    wider = lambda a: a.astype(jnp.float32)
    narrower = lambda a: a.astype(jnp.bfloat16)
    back = [[(i, (i - k) % groups) for i in range(groups)] for k in range(groups)]
    first = FIRST_PART * rows
    halves = [slice(0, first), slice(first, unit)]
    from_core = [lax.ppermute(sums[4 * k], "wide", to_core) for k in range(groups)]

    def column_part(k, half):
        away = wider(from_core[k][unit:][half])
        return wider(sums[4 * k + 1][half]) + jnp.where(for_column, away, zero)

    def side_part(k, half):
        away = wider(from_core[k][unit:][half])
        return wider(sums[4 * k + 2][half]) + jnp.where(for_column, zero, away)

    column_sent = []
    for half in halves:
        column_sent.append(
            [
                lax.ppermute(narrower(column_part(k, half)), "narrow", back[k])
                for k in range(1, groups)
            ]
        )
    other_side = [
        lax.ppermute(narrower(side_part(k, slice(0, unit))), "wide", to_side)
        for k in range(1, groups)
    ]
    from_column = []
    for half, received in zip(halves, column_sent):
        column = column_part(0, half)
        for piece in received:
            column = column + wider(piece)
        from_column.append(lax.ppermute(narrower(column), "wide", to_column))
    from_narrow = []
    for k in range(1, groups):
        total = wider(sums[4 * k + 3]) + wider(from_core[k][:unit]) + wider(other_side[k - 1])
        from_narrow.append(lax.ppermute(narrower(total), "narrow", back[k]))
    from_side = []
    for half, piece in zip(halves, from_column):
        part = narrower(side_part(0, half) + wider(piece))
        from_side.append(lax.ppermute(part, "wide", to_side))
    final = [sums[3], from_core[0]] + from_narrow
    return divided(final, from_side, part_levels, field_vars, rows, in_kernel)


def solution(mesh):
    placed = (
        P(None, "narrow", "wide"),
        P(("wide", "narrow")),
        P(("wide", "narrow"), None, None),
        P(("wide", "narrow")),
        P(("wide", "narrow")),
        P(("wide", "narrow")),
    )
    return jax.shard_map(
        per_device, mesh=mesh, in_specs=placed, out_specs=P(None, "narrow", "wide"), check_vma=False
    )
```
